256 devices in a mesh: leaf: 256 (over z, y, x, core).
Axes of the slice: x: 4, y: 4, z: 8, core: 2. Of those that a mesh axis runs over, the one named last changes fastest.
Arguments:
- panels: bfloat16 [512, 64, 256], P('leaf'), may hold values from -6 to 6
- basis: bfloat16 [512, 64, 256], P('leaf'), may hold values from -0.375 to 0.375
- transfer: bfloat16 [512, 64, 64], P('leaf'), may hold values from -0.25 to 0.25
- near_blocks: bfloat16 [512, 27, 256, 256], P('leaf'), may hold values from -0.078125 to 0.078125
- coupling: bfloat16 [2, 343, 4096], replicated, may hold values from -0.0546875 to 0.0546875
- near_list: int32 [512, 27], P('leaf'), may hold values from -1 to 511, as said below
Outputs:
- product: bfloat16 [512, 64, 256], P('leaf')
The draws below stay inside these ranges and needn't reach their ends.
Inputs may be any that keep to these rules, and one draw needn't show every extreme that they name: `near_list`: row i lists, in an order of no meaning, leaf i and the leaves whose grid positions differ from it by at most one in each coordinate; -1 fills the other slots.
All inputs are finite; a program needn't handle non-finite values.
Results may differ from the reference program's by a relative error of at most 0.0035.
Values may be sent and summed in bfloat16 or wider, within the bound.
A program may use at most 192 MiB of HBM per device.

```python
import jax
import jax.numpy as jnp
from jax import lax

LEAF = 256
RANK = 64
COLS = 64
NNEAR = 27
SHIFTS = 343
LEAVES = 512
CLUSTERS = 64


def decode_drawn(indices, bit_count):
    coords = [jnp.zeros_like(indices) for a in range(3)]
    for k in range(bit_count):
        coords[k % 3] = coords[k % 3] + ((indices >> k & 1) << k // 3)
    return coords


def encode_drawn(coords, bit_count):
    result = jnp.zeros_like(coords[0])
    for k in range(bit_count):
        result = result + ((coords[k % 3] >> k // 3 & 1) << k)
    return result


def grid_extent_drawn(bit_count):
    return [2 ** len([k for k in range(bit_count) if k % 3 == a]) for a in range(3)]


def shuffle_rows(key, table, width):
    column = jnp.arange(table.shape[1], dtype=jnp.int32)[None, :]
    noise = jax.random.randint(key, table.shape, 0, 1 << 20, dtype=jnp.int32)
    score = jnp.where(table >= 0, 1 << 29, 0) + noise * 256 + column
    order = jnp.argsort(-score, axis=1)
    return jnp.take_along_axis(table, order, axis=1)[:, :width].astype(jnp.int32)


def near_rows(key, bit_count):
    count = 2 ** bit_count
    coords = decode_drawn(jnp.arange(count, dtype=jnp.int32), bit_count)
    extent = grid_extent_drawn(bit_count)
    entries = []
    for delta in [(a, b, c) for a in (-1, 0, 1) for b in (-1, 0, 1) for c in (-1, 0, 1)]:
        moved = [coords[a] + delta[a] for a in range(3)]
        inside = (moved[0] >= 0) & (moved[0] < extent[0]) & (moved[1] >= 0) & (moved[1] < extent[1]) & (moved[2] >= 0) & (moved[2] < extent[2])
        entries.append(jnp.where(inside, encode_drawn(moved, bit_count), -1))
    return shuffle_rows(key, jnp.stack(entries, axis=1), NNEAR)


def draw_near_list(key, part):
    return near_rows(jax.random.fold_in(key, 11), int(LEAVES).bit_length() - 1)


def levels(rng, shape, cuts, smallest, largest):
    level = 1.0
    for dim, shards_of in cuts:
        heights = jax.random.uniform(jax.random.fold_in(jax.random.fold_in(rng, 6), dim), (shards_of,), jnp.float32, smallest / len(cuts), largest / len(cuts))
        level = level * jnp.repeat(jnp.exp(heights), shape[dim] // shards_of).reshape((-1,) + (1,) * (len(shape) - 1 - dim))
    return level


def centred(stream_key, shape, spread, bound, split=(), kind=jnp.bfloat16):
    loudness = levels(stream_key, shape, split, -0.22, 0.18) if split else 1.0
    values = jax.random.normal(stream_key, shape, jnp.float32) * spread * loudness
    return jnp.minimum(jnp.maximum(values, -bound), bound).astype(kind)


def setup_inputs(seed: int = 0) -> dict:
    streams_of = jax.random.split(jax.random.key(seed), 7)
    return {
        "panels": centred(streams_of[0], (LEAVES, COLS, LEAF), 1.0, 6.0, ((0, 256),)),
        "basis": centred(streams_of[1], (LEAVES, RANK, LEAF), LEAF ** -0.5, 0.375, ((0, 256),)),
        "transfer": centred(streams_of[2], (LEAVES, RANK, RANK), (8 * RANK) ** -0.5, 0.25, ((0, 256),)),
        "near_blocks": centred(streams_of[3], (LEAVES, NNEAR, LEAF, LEAF), (NNEAR * LEAF) ** -0.5, 0.078125, ((0, 256),)),
        "coupling": centred(streams_of[4], (2, SHIFTS, RANK * RANK), (189 * RANK) ** -0.5, 0.0546875),
        "near_list": draw_near_list(jax.random.fold_in(streams_of[6], 71), 0),
    }


def decode(indices, bit_count):
    coords = [jnp.zeros_like(indices) for a in range(3)]
    for k in range(bit_count):
        coords[k % 3] = coords[k % 3] + (((indices >> k) & 1) << (k // 3))
    return coords


def encode(coords, bit_count):
    result = jnp.zeros_like(coords[0])
    for k in range(bit_count):
        result = result + (((coords[k % 3] >> (k // 3)) & 1) << k)
    return result


def grid_extent(bit_count):
    return [2 ** len([k for k in range(bit_count) if k % 3 == a]) for a in range(3)]


def far_table(cells, bit_count):
    coords = decode(cells, bit_count)
    extent = grid_extent(bit_count)
    entries = []
    for delta in [(a, b, c) for a in (-1, 0, 1) for b in (-1, 0, 1) for c in (-1, 0, 1)]:
        upper = [(coords[a] >> 1) + delta[a] for a in range(3)]
        inside = (upper[0] >= 0) & (upper[0] < extent[0] // 2) & (upper[1] >= 0) & (upper[1] < extent[1] // 2) & (upper[2] >= 0) & (upper[2] < extent[2] // 2)
        for child in [(a, b, c) for a in (0, 1) for b in (0, 1) for c in (0, 1)]:
            moved = [2 * upper[a] + child[a] for a in range(3)]
            apart = (jnp.abs(moved[0] - coords[0]) > 1) | (jnp.abs(moved[1] - coords[1]) > 1) | (jnp.abs(moved[2] - coords[2]) > 1)
            entries.append(jnp.where(inside & apart, encode(moved, bit_count), -1))
    return jnp.stack(entries, axis=-1).astype(jnp.int32)


def shift_code(targets, sources, bit_count):
    safe = jnp.maximum(sources, 0)
    first = decode(targets, bit_count)
    second = decode(safe, bit_count)
    return (49 * (second[0] - first[0] + 3) + 7 * (second[1] - first[1] + 3) + (second[2] - first[2] + 3)).astype(jnp.int32)


def couple(coef_table, table, rows, codes):
    valid = (rows >= 0).astype(jnp.float32)
    picked = jnp.take(coef_table, jnp.maximum(rows, 0), axis=0).astype(jnp.float32) * valid[:, None, None]
    mats = jnp.take(table, codes, axis=0).astype(jnp.float32).reshape(rows.shape[0], RANK, RANK)
    return jnp.einsum('jcr,jrs->cs', picked, mats)


def reference(panels, basis, transfer, near_blocks, coupling, near_list):
    bit_count = int(LEAVES).bit_length() - 1
    leaf_coef = jnp.einsum('lcq,lrq->lcr', panels.astype(jnp.float32), basis.astype(jnp.float32)).astype(jnp.bfloat16)
    partial_value = jnp.einsum('lcr,lrs->lcs', leaf_coef.astype(jnp.float32), transfer.astype(jnp.float32))
    cluster_coef = partial_value.reshape(CLUSTERS, 8, COLS, RANK).sum(axis=1).astype(jnp.bfloat16)
    leaf_ids = jnp.arange(LEAVES, dtype=jnp.int32)
    cluster_ids = jnp.arange(CLUSTERS, dtype=jnp.int32)
    far_leaf = far_table(leaf_ids, bit_count)
    far_cluster = far_table(cluster_ids, bit_count - 3)
    codes_leaf = shift_code(leaf_ids[:, None], far_leaf, bit_count)
    codes_cluster = shift_code(cluster_ids[:, None], far_cluster, bit_count - 3)
    down_coef = lax.map(lambda item: couple(cluster_coef, coupling[1], item[0], item[1]), (far_cluster, codes_cluster)).astype(jnp.bfloat16)
    leaf_far = lax.map(lambda item: couple(leaf_coef, coupling[0], item[0], item[1]), (far_leaf, codes_leaf))
    parent_down = jnp.repeat(down_coef, 8, axis=0).astype(jnp.float32)
    far_coef = (leaf_far + jnp.einsum('lcs,lrs->lcr', parent_down, transfer.astype(jnp.float32))).astype(jnp.bfloat16)
    far_term = jnp.einsum('lcr,lrq->lcq', far_coef.astype(jnp.float32), basis.astype(jnp.float32))

    def near_one(item):
        rows, blocks = item
        valid = (rows >= 0).astype(jnp.float32)
        picked = jnp.take(panels, jnp.maximum(rows, 0), axis=0).astype(jnp.float32) * valid[:, None, None]
        return jnp.einsum('kcq,kqp->cp', picked, blocks.astype(jnp.float32))

    near = lax.map(near_one, (near_list, near_blocks))
    return (near + far_term).astype(jnp.bfloat16)
```

```python
import jax
import jax.numpy as jnp
from jax import lax
from jax.experimental import pallas as pl
from jax.experimental.pallas import tpu as pltpu
from jax.sharding import PartitionSpec as P

MESH = pl.DeviceIdType.MESH
AXIS = "leaf"
LEAF = 256
RANK = 64
COLS = 64
NNEAR = 27
SHIFTS = 343
HALF = RANK // 2
PAIR = 2 * COLS
ZERO_SLOT = 36
GROUP = 7


def bit(value, k):
    return (value // (1 << k)) % 2


def device_position(dev):
    bx = bit(dev, 2) + 2 * bit(dev, 5)
    y = bit(dev, 0) + 2 * bit(dev, 3) + 4 * bit(dev, 6)
    z = bit(dev, 1) + 2 * bit(dev, 4) + 4 * bit(dev, 7)
    return bx, y, z


def device_at(bx, y, z):
    return (
        y % 2
        + 2 * (z % 2)
        + 4 * (bx % 2)
        + 8 * ((y // 2) % 2)
        + 16 * ((z // 2) % 2)
        + 32 * (bx // 2)
        + 64 * (y // 4)
        + 128 * (z // 4)
    )


def cluster_position(p):
    px = bit(p, 0) + 2 * bit(p, 3)
    py = bit(p, 1) + 2 * bit(p, 4)
    pz = bit(p, 2) + 2 * bit(p, 5)
    return px, py, pz


def cluster_at(px, py, pz):
    return (
        px % 2
        + 2 * (py % 2)
        + 4 * (pz % 2)
        + 8 * (px // 2)
        + 16 * (py // 2)
        + 32 * (pz // 2)
    )


def within(value, size):
    return (value >= 0) & (value < size)


def split_rows(scratch, value):
    scratch[...] = value
    even = scratch[pl.ds(0, HALF, stride=2), :]
    odd = scratch[pl.ds(1, HALF, stride=2), :]
    return jnp.concatenate([even, odd], axis=1)


def split_levels(raw, turn, tables):
    group = turn.shape[0] // RANK

    def split(i, carry):
        first = i * group
        turn[...] = raw[pl.ds(first, group)].reshape(group * RANK, PAIR).astype(jnp.float32)
        for level, table in enumerate(tables):
            rows = turn[pl.ds(level, group * HALF, stride=2), :]
            table[pl.ds(first, group)] = rows.astype(jnp.bfloat16).reshape(group, HALF, PAIR)
        return carry

    lax.fori_loop(0, SHIFTS // group, split, 0)


def kernel(
    panels_ref,
    basis_ref,
    transfer_ref,
    near_ref,
    coupling_ref,
    list_ref,
    out_ref,
    pbuf,
    nbuf,
    basis_vmem,
    transfer_vmem,
    raw,
    m0,
    m1,
    x0,
    x1,
    x1_own,
    cluster_send,
    cluster_recv,
    sum_send,
    sum_recv,
    tmp,
    turn,
    xt,
    load_sem,
    panel_send_sem,
    panel_recv_sem,
    coef_send_sem,
    coef_recv_sem,
    part_send_sem,
    part_recv_sem,
    clus_send_sem,
    clus_recv_sem,
    sum_send_sem,
    sum_recv_sem,
):
    me = lax.axis_index(AXIS)
    g = me % 4
    gy = me % 2
    gz = (me // 2) % 2
    parent = me // 4
    bx, y, z = device_position(me)
    px, py, pz = cluster_position(parent)
    own_slot = 17

    load_panels = pltpu.make_async_copy(panels_ref, pbuf.at[pl.ds(own_slot, 2)], load_sem.at[0])
    load_panels.start()
    load_basis = pltpu.make_async_copy(basis_ref, basis_vmem, load_sem.at[1])
    load_basis.start()
    load_transfer = pltpu.make_async_copy(transfer_ref, transfer_vmem, load_sem.at[2])
    load_transfer.start()
    load_raw = pltpu.make_async_copy(coupling_ref, raw, load_sem.at[3])
    load_raw.start()
    load_near = pltpu.make_async_copy(near_ref, nbuf, load_sem.at[4])
    load_near.start()

    x0[...] = jnp.zeros_like(x0)
    x1[...] = jnp.zeros_like(x1)
    pbuf[ZERO_SLOT] = jnp.zeros((COLS, LEAF), jnp.bfloat16)

    def panel_partner(i):
        ox, oy, oz = i // 9 - 1, (i // 3) % 3 - 1, i % 3 - 1
        tx, ty, tz = bx + ox, y + oy, z + oz
        there = within(tx, 4) & within(ty, 8) & within(tz, 8) & (i != 13)
        return device_at(tx, ty, tz), there, ox, oy, oz

    def coef_partner(i):
        tx, ty, tz = px + i // 9 - 1, py + (i // 3) % 3 - 1, pz + i % 3 - 1
        there = within(tx, 4) & within(ty, 4) & within(tz, 4) & (i != 13)
        return 4 * cluster_at(tx, ty, tz) + g, there

    def cluster_far(other):
        qx, qy, qz = cluster_position(other)
        dx, dy, dz = qx - px, qy - py, qz - pz
        near = within(dx + 1, 3) & within(dy + 1, 3) & within(dz + 1, 3)
        return jnp.logical_not(near)

    barrier = pltpu.get_barrier_semaphore()

    def greet(dev, there):
        @pl.when(there)
        def _():
            pl.semaphore_signal(barrier, inc=1, device_id=(dev,), device_id_type=MESH)

        return jnp.where(there, 1, 0)

    def greet_near(i, count):
        dev, there, _, _, _ = panel_partner(i)
        count = count + greet(dev, there)
        dev, there = coef_partner(i)
        return count + greet(dev, there)

    def greet_cluster(i, count):
        return count + greet(4 * (4 * i + g) + parent % 4, cluster_far(4 * i + g))

    count = lax.fori_loop(0, 27, greet_near, 0)
    count = lax.fori_loop(0, 16, greet_cluster, count)
    for r in range(1, 4):
        pl.semaphore_signal(
            barrier, inc=1, device_id=(4 * parent + (g + r) % 4,), device_id_type=MESH
        )
    count = count + 3

    load_panels.wait()
    load_basis.wait()
    load_transfer.wait()
    part = jnp.zeros((RANK, COLS), jnp.float32)
    for h in range(2):
        coef = lax.dot_general(
            basis_vmem[h],
            pbuf[own_slot + h],
            (((1,), (1,)), ((), ())),
            preferred_element_type=jnp.float32,
        )
        x0[13, pl.ds(HALF * h, HALF), :] = split_rows(tmp, coef).astype(jnp.bfloat16)
        part = part + lax.dot_general(
            transfer_vmem[h],
            coef.astype(jnp.bfloat16),
            (((0,), (0,)), ((), ())),
            preferred_element_type=jnp.float32,
        )
    cluster_send[...] = split_rows(tmp, part)

    pl.semaphore_wait(barrier, count)

    def part_copy(r):
        return pltpu.make_async_remote_copy(
            src_ref=cluster_send,
            dst_ref=cluster_recv.at[r - 1],
            send_sem=part_send_sem.at[r - 1],
            recv_sem=part_recv_sem.at[r - 1],
            device_id=(4 * parent + (g + r) % 4,),
            device_id_type=MESH,
        )

    for r in range(1, 4):
        part_copy(r).start()

    def coef_copy(i, slot, dev):
        return pltpu.make_async_remote_copy(
            src_ref=x0.at[13],
            dst_ref=x0.at[slot],
            send_sem=coef_send_sem.at[i],
            recv_sem=coef_recv_sem.at[slot],
            device_id=(dev,),
            device_id_type=MESH,
        )

    def send_coef(i, carry):
        dev, there = coef_partner(i)

        @pl.when(there)
        def _():
            coef_copy(i, 26 - i, dev).start()

        return carry

    lax.fori_loop(0, 27, send_coef, 0)

    def panel_copy(i, dev, leaf, leaves, slot):
        return pltpu.make_async_remote_copy(
            src_ref=pbuf.at[pl.ds(own_slot + leaf, leaves)],
            dst_ref=pbuf.at[pl.ds(slot, leaves)],
            send_sem=panel_send_sem.at[i],
            recv_sem=panel_recv_sem.at[26 - i],
            device_id=(dev,),
            device_id_type=MESH,
        )

    x_steps = ((0, 1, 3), (0, 2, 1), (1, 1, 0))

    def send_panel(j, carry):
        for step, (leaf, leaves, place) in enumerate(x_steps):
            i = 9 * step + j
            dev, there, _, oy, oz = panel_partner(i)

            @pl.when(there)
            def _():
                slot = ((1 - oz) * 3 + 1 - oy) * 4 + place
                panel_copy(i, dev, leaf, leaves, slot).start()

        return carry

    for r in range(1, 4):
        part_copy(r).wait_recv()
    total = cluster_send[...] + cluster_recv[0] + cluster_recv[1] + cluster_recv[2]
    x1_own[...] = total.astype(jnp.bfloat16)

    def clus_copy(i, slot, dev):
        return pltpu.make_async_remote_copy(
            src_ref=x1_own,
            dst_ref=x1.at[slot],
            send_sem=clus_send_sem.at[i],
            recv_sem=clus_recv_sem.at[slot],
            device_id=(dev,),
            device_id_type=MESH,
        )

    def send_cluster(i, carry):
        @pl.when(cluster_far(4 * i + g))
        def _():
            clus_copy(i, parent // 4, 4 * (4 * i + g) + parent % 4).start()

        return carry

    lax.fori_loop(0, 16, send_cluster, 0)
    lax.fori_loop(0, 9, send_panel, 0)

    load_raw.wait()
    split_levels(raw, turn, (m0, m1))
    for table in (m0, m1):
        for dx in (2, 3, 4):
            for dy in (2, 3, 4):
                first = 49 * dx + 7 * dy + 2
                table[pl.ds(first, 3)] = jnp.zeros((3, HALF, PAIR), jnp.bfloat16)

    def wait_coef(i, carry):
        _, there = coef_partner(i)

        @pl.when(there)
        def _():
            coef_copy(i, i, me).wait_recv()

        return carry

    lax.fori_loop(0, 27, wait_coef, 0)
    offsets = [(a, b, c) for a in (-1, 0, 1) for b in (-1, 0, 1) for c in (-1, 0, 1)]
    chunks = [list(range(first, min(first + 4, 27))) for first in range(0, 27, 4)]
    for t, chunk in enumerate(chunks):
        rows = x0[pl.ds(chunk[0], len(chunk))].reshape(len(chunk) * RANK, PAIR)
        xt[t, :, : len(chunk) * RANK] = rows.T
    lanes = lax.broadcasted_iota(jnp.int32, (COLS, PAIR), 1)
    base = 7 * gy + gz
    for tz in range(2):
        for ty in range(2):
            acc = jnp.zeros((PAIR, 2 * PAIR), jnp.float32)
            for t, chunk in enumerate(chunks):
                columns = []
                for tx in range(2):
                    column = []
                    for e in chunk:
                        ex, ey, ez = offsets[e]
                        for h in range(2):
                            code = (
                                49 * (2 * ex + h - tx + 3)
                                + 7 * (2 * ey - ty + 3)
                                + (2 * ez - tz + 3)
                            )
                            column.append(m0[base + code])
                    columns.append(jnp.concatenate(column, axis=0))
                weights = jnp.concatenate(columns, axis=1)
                acc = acc + jnp.dot(
                    xt[t, :, : len(chunk) * RANK], weights, preferred_element_type=jnp.float32
                )
            first = acc[:COLS, :PAIR] + pltpu.roll(acc[COLS:, :PAIR], COLS, 1)
            second = pltpu.roll(acc[:COLS, PAIR:], COLS, 1) + acc[COLS:, PAIR:]
            sum_send[2 * tz + ty, :COLS, :] = jnp.where(lanes < COLS, first, second)

    def wait_cluster(i, carry):
        @pl.when(cluster_far(4 * i + g))
        def _():
            clus_copy(i, i, me).wait_recv()

        return carry

    lax.fori_loop(0, 16, wait_cluster, 0)
    acc = jnp.zeros((PAIR, PAIR), jnp.float32)
    for t in range(2):
        column = []
        for i in range(8 * t, 8 * t + 8):
            qx, qy, qz = cluster_position(4 * i + g)
            column.append(m1[49 * (qx - px + 3) + 7 * (qy - py + 3) + (qz - pz + 3)])
        rows = x1[pl.ds(8 * t, 8)].reshape(8 * HALF, PAIR)
        acc = acc + jnp.dot(
            rows.T, jnp.concatenate(column, axis=0), preferred_element_type=jnp.float32
        )
    down = acc[:COLS] + pltpu.roll(acc[COLS:], COLS, 1)
    down = jnp.where(lanes[:HALF] < COLS, down[:HALF], pltpu.roll(down[HALF:], COLS, 1))
    for n in range(4):
        sum_send[n, COLS:, :] = down

    def sum_copy(r):
        return pltpu.make_async_remote_copy(
            src_ref=sum_send.at[(g + r) % 4],
            dst_ref=sum_recv.at[r - 1],
            send_sem=sum_send_sem.at[r - 1],
            recv_sem=sum_recv_sem.at[r - 1],
            device_id=(4 * parent + (g + r) % 4,),
            device_id_type=MESH,
        )

    for r in range(1, 4):
        sum_copy(r).start()

    def wait_panel(j, carry):
        for step, (leaf, leaves, place) in enumerate(x_steps):
            i = 9 * step + j
            _, there, _, oy, oz = panel_partner(i)

            @pl.when(there)
            def _():
                slot = ((1 - oz) * 3 + 1 - oy) * 4 + place
                panel_copy(26 - i, me, 0, leaves, slot).wait_recv()

        return carry

    lax.fori_loop(0, 9, wait_panel, 0)
    load_near.wait()

    def slot_of(entry):
        lx = ((entry >> 0) & 1) + 2 * ((entry >> 3) & 1) + 4 * ((entry >> 6) & 1)
        ly = ((entry >> 1) & 1) + 2 * ((entry >> 4) & 1) + 4 * ((entry >> 7) & 1)
        lz = ((entry >> 2) & 1) + 2 * ((entry >> 5) & 1) + 4 * ((entry >> 8) & 1)
        slot = ((lz - z + 1) * 3 + ly - y + 1) * 4 + lx - 2 * bx + 1
        return jnp.where(entry < 0, ZERO_SLOT, jnp.clip(slot, 0, ZERO_SLOT))

    near_terms = []
    for h in range(2):
        acc = jnp.zeros((COLS, LEAF), jnp.float32)
        for k in range(NNEAR):
            acc = acc + jnp.dot(
                pbuf[slot_of(list_ref[h, k])], nbuf[h, k], preferred_element_type=jnp.float32
            )
        near_terms.append(acc)

    for r in range(1, 4):
        sum_copy(r).wait_recv()
    sums = sum_send[g] + sum_recv[0] + sum_recv[1] + sum_recv[2]
    down = jnp.concatenate([sums[COLS:, :COLS], sums[COLS:, COLS:]], axis=0).astype(jnp.bfloat16)
    for h in range(2):
        far_coef = sums[:COLS, COLS * h : COLS * (h + 1)] + lax.dot_general(
            down,
            transfer_vmem[h],
            (((1,), (1,)), ((), ())),
            preferred_element_type=jnp.float32,
        )
        far_term = jnp.dot(
            far_coef.astype(jnp.bfloat16), basis_vmem[h], preferred_element_type=jnp.float32
        )
        out_ref[h] = (near_terms[h] + far_term).astype(jnp.bfloat16)

    for r in range(1, 4):
        part_copy(r).wait_send()
        sum_copy(r).wait_send()

    def drain(i, carry):
        dev, there = coef_partner(i)

        @pl.when(there)
        def _():
            coef_copy(i, 26 - i, dev).wait_send()

        return carry

    lax.fori_loop(0, 27, drain, 0)

    def drain_cluster(i, carry):
        @pl.when(cluster_far(4 * i + g))
        def _():
            clus_copy(i, parent // 4, 4 * (4 * i + g) + parent % 4).wait_send()

        return carry

    lax.fori_loop(0, 16, drain_cluster, 0)

    def drain_panel(j, carry):
        for step, (leaf, leaves, place) in enumerate(x_steps):
            i = 9 * step + j
            dev, there, _, oy, oz = panel_partner(i)

            @pl.when(there)
            def _():
                slot = ((1 - oz) * 3 + 1 - oy) * 4 + place
                panel_copy(i, dev, leaf, leaves, slot).wait_send()

        return carry

    lax.fori_loop(0, 9, drain_panel, 0)


def per_device(panels, basis, transfer, near_blocks, coupling, near_list):
    tables = coupling.reshape(2, SHIFTS, HALF, PAIR).transpose(1, 2, 0, 3)
    tables = tables.reshape(SHIFTS, RANK, PAIR)
    vmem = pl.BlockSpec(memory_space=pltpu.VMEM)
    hbm = pl.BlockSpec(memory_space=pltpu.HBM)
    dma = pltpu.SemaphoreType.DMA
    return pl.pallas_call(
        kernel,
        name="h2_product",
        out_shape=jax.ShapeDtypeStruct((2, COLS, LEAF), jnp.bfloat16),
        in_specs=[hbm, hbm, hbm, hbm, hbm, pl.BlockSpec(memory_space=pltpu.SMEM)],
        out_specs=vmem,
        scratch_shapes=[
            pltpu.VMEM((37, COLS, LEAF), jnp.bfloat16),
            pltpu.VMEM((2, NNEAR, LEAF, LEAF), jnp.bfloat16),
            pltpu.VMEM((2, RANK, LEAF), jnp.bfloat16),
            pltpu.VMEM((2, RANK, RANK), jnp.bfloat16),
            pltpu.VMEM((SHIFTS, RANK, PAIR), jnp.bfloat16),
            pltpu.VMEM((SHIFTS, HALF, PAIR), jnp.bfloat16),
            pltpu.VMEM((SHIFTS, HALF, PAIR), jnp.bfloat16),
            pltpu.VMEM((27, RANK, PAIR), jnp.bfloat16),
            pltpu.VMEM((16, HALF, PAIR), jnp.bfloat16),
            pltpu.VMEM((HALF, PAIR), jnp.bfloat16),
            pltpu.VMEM((HALF, PAIR), jnp.float32),
            pltpu.VMEM((3, HALF, PAIR), jnp.float32),
            pltpu.VMEM((4, COLS + HALF, PAIR), jnp.float32),
            pltpu.VMEM((3, COLS + HALF, PAIR), jnp.float32),
            pltpu.VMEM((RANK, COLS), jnp.float32),
            pltpu.VMEM((GROUP * RANK, PAIR), jnp.float32),
            pltpu.VMEM((7, PAIR, 2 * PAIR), jnp.bfloat16),
            dma((5,)),
            dma((27,)),
            dma((27,)),
            dma((27,)),
            dma((27,)),
            dma((3,)),
            dma((3,)),
            dma((16,)),
            dma((16,)),
            dma((3,)),
            dma((3,)),
        ],
        compiler_params=pltpu.CompilerParams(
            collective_id=0, has_side_effects=True, vmem_limit_bytes=56 << 20
        ),
    )(panels, basis, transfer, near_blocks, tables, near_list)


def solution(mesh):
    return jax.shard_map(
        per_device,
        mesh=mesh,
        in_specs=(
            P(AXIS, None, None),
            P(AXIS, None, None),
            P(AXIS, None, None),
            P(AXIS, None, None, None),
            P(),
            P(AXIS, None),
        ),
        out_specs=P(AXIS, None, None),
        check_vma=False,
    )
```

```python
import jax
import jax.numpy as jnp
from jax import lax
from jax.experimental import pallas as pl
from jax.experimental.pallas import tpu as pltpu
from jax.sharding import PartitionSpec as P

MESH = pl.DeviceIdType.MESH
AXIS = "leaf"
LEAF = 256
RANK = 64
COLS = 64
NNEAR = 27
SHIFTS = 343
HALF = RANK // 2
PAIR = 2 * COLS
ZERO_SLOT = 36
GROUP = 7


def bit(value, k):
    return (value // (1 << k)) % 2


def device_position(dev):
    bx = bit(dev, 2) + 2 * bit(dev, 5)
    y = bit(dev, 0) + 2 * bit(dev, 3) + 4 * bit(dev, 6)
    z = bit(dev, 1) + 2 * bit(dev, 4) + 4 * bit(dev, 7)
    return bx, y, z


def cluster_position(p):
    px = bit(p, 0) + 2 * bit(p, 3)
    py = bit(p, 1) + 2 * bit(p, 4)
    pz = bit(p, 2) + 2 * bit(p, 5)
    return px, py, pz


OFFSETS = [(a, b, c) for a in (-1, 0, 1) for b in (-1, 0, 1) for c in (-1, 0, 1)]
CENTRE = 13


def neighbours(position, sizes, weights):
    axes = []
    for here, size, bits in zip(position, sizes, weights):
        steps = {}
        for step in (-1, 0, 1):
            there = here + step
            share = sum(weight * bit(there, k) for k, weight in enumerate(bits))
            steps[step] = (share, {-1: here > 0, 0: None, 1: here < size - 1}[step])
        axes.append(steps)
    found = []
    for offset in OFFSETS:
        parts = [axes[a][offset[a]] for a in range(3)]
        valid = [ok for _, ok in parts if ok is not None]
        there = None
        for ok in valid:
            there = ok if there is None else there & ok
        found.append((sum(share for share, _ in parts), there))
    total = 1
    for here, size in zip(position, sizes):
        total = total * (1 + jnp.where(here > 0, 1, 0) + jnp.where(here < size - 1, 1, 0))
    return found, total - 1


def split_rows(scratch, value):
    scratch[...] = value
    even = scratch[pl.ds(0, HALF, stride=2), :]
    odd = scratch[pl.ds(1, HALF, stride=2), :]
    return jnp.concatenate([even, odd], axis=1)


def split_levels(raw, turn, tables):
    group = turn.shape[0] // RANK

    def split(i, carry):
        first = i * group
        turn[...] = raw[pl.ds(first, group)].reshape(group * RANK, PAIR).astype(jnp.float32)
        for level, table in enumerate(tables):
            rows = turn[pl.ds(level, group * HALF, stride=2), :]
            table[pl.ds(first, group)] = rows.astype(jnp.bfloat16).reshape(group, HALF, PAIR)
        return carry

    lax.fori_loop(0, SHIFTS // group, split, 0)


def kernel(
    panels_ref,
    basis_ref,
    transfer_ref,
    near_ref,
    coupling_ref,
    list_hbm,
    out_ref,
    pbuf,
    nbuf,
    list_ref,
    basis_vmem,
    transfer_vmem,
    raw,
    m0,
    m1,
    x0,
    x1,
    x1_own,
    cluster_send,
    cluster_recv,
    sum_send,
    sum_recv,
    tmp,
    turn,
    xt,
    load_sem,
    panel_send_sem,
    panel_recv_sem,
    coef_send_sem,
    coef_recv_sem,
    part_send_sem,
    part_recv_sem,
    clus_send_sem,
    clus_recv_sem,
    sum_send_sem,
    sum_recv_sem,
):
    me = lax.axis_index(AXIS)
    g = me % 4
    gy = me % 2
    gz = (me // 2) % 2
    parent = me // 4
    bx, y, z = device_position(me)
    px, py, pz = cluster_position(parent)
    own_slot = 17

    load_panels = pltpu.make_async_copy(panels_ref, pbuf.at[pl.ds(own_slot, 2)], load_sem.at[0])
    load_panels.start()
    load_basis = pltpu.make_async_copy(basis_ref, basis_vmem, load_sem.at[1])
    load_basis.start()
    load_transfer = pltpu.make_async_copy(transfer_ref, transfer_vmem, load_sem.at[2])
    load_transfer.start()
    load_list = pltpu.make_async_copy(list_hbm, list_ref, load_sem.at[5])
    load_list.start()
    load_raw = pltpu.make_async_copy(coupling_ref, raw, load_sem.at[3])
    load_raw.start()
    load_near = pltpu.make_async_copy(near_ref, nbuf, load_sem.at[4])
    load_near.start()

    x0[...] = jnp.zeros_like(x0)
    x1[...] = jnp.zeros_like(x1)
    pbuf[ZERO_SLOT] = jnp.zeros((COLS, LEAF), jnp.bfloat16)

    def ones(flags):
        return sum(jnp.where(flag, 1, 0) for flag in flags)

    def place_of(position):
        tx, ty, tz = position
        share_x = 4 * bit(tx, 0) + 32 * bit(tx, 1)
        share_y = bit(ty, 0) + 8 * bit(ty, 1) + 64 * bit(ty, 2)
        share_z = 2 * bit(tz, 0) + 16 * bit(tz, 1) + 128 * bit(tz, 2)
        return share_x + share_y + share_z

    side_x = [(place_of((bx + d, y, z)), ok) for d, ok in ((-1, bx > 0), (1, bx < 3))]
    side_y = [(place_of((bx, y + d, z)), ok) for d, ok in ((-1, y > 0), (1, y < 7))]
    side_z = [(place_of((bx, y, z + d)), ok) for d, ok in ((-1, z > 0), (1, z < 7))]
    panel_count = ones([ok for _, ok in side_x + side_y + side_z])
    coef_partners, coef_count = neighbours(
        (px, py, pz), (4, 4, 4), ((4, 32), (8, 64), (16, 128))
    )
    coef_partners = [(dev + g, there) for dev, there in coef_partners]

    def close(q, p):
        return (q - p < 2) & (p - q < 2)

    near_x = [close(gy + 2 * k, px) for k in range(2)]
    near_y = [close(gz + 2 * k, py) for k in range(2)]
    near_z = [close(k, pz) for k in range(4)]
    clusters = []
    for i in range(16):
        kx, ky, kz = (i // 2) % 2, (i // 4) % 2, i % 2 + 2 * (i // 8)
        near = near_x[kx] & near_y[ky] & near_z[kz]
        dev = 16 * i + 4 * g + parent % 4
        clusters.append((dev, jnp.logical_not(near), 98 * kx + 14 * ky + kz))
    cluster_base = 49 * (gy - px + 3) + 7 * (gz - py + 3) + 3 - pz

    cluster_count = 16 - ones(near_x) * ones(near_y) * ones(near_z)
    mates = [4 * parent + (g + r) % 4 for r in range(1, 4)]

    def for_each(partners, action):
        for i, partner in enumerate(partners):
            if partner[1] is None:
                continue

            @pl.when(partner[1])
            def _():
                action(i, partner[0])

    barrier = pltpu.get_barrier_semaphore()

    def greet(i, dev):
        pl.semaphore_signal(barrier, inc=1, device_id=(dev,), device_id_type=MESH)

    for dev in mates:
        greet(0, dev)
    for_each(side_x + side_y + side_z, greet)
    for_each(coef_partners, greet)
    for_each(clusters, greet)
    count = panel_count + coef_count + cluster_count + 3

    load_panels.wait()
    load_basis.wait()
    load_transfer.wait()
    part = jnp.zeros((RANK, COLS), jnp.float32)
    for h in range(2):
        coef = lax.dot_general(
            basis_vmem[h],
            pbuf[own_slot + h],
            (((1,), (1,)), ((), ())),
            preferred_element_type=jnp.float32,
        )
        x0[13, pl.ds(HALF * h, HALF), :] = split_rows(tmp, coef).astype(jnp.bfloat16)
        part = part + lax.dot_general(
            transfer_vmem[h],
            coef.astype(jnp.bfloat16),
            (((0,), (0,)), ((), ())),
            preferred_element_type=jnp.float32,
        )
    cluster_send[...] = split_rows(tmp, part)

    pl.semaphore_wait(barrier, count)

    def part_copy(r):
        return pltpu.make_async_remote_copy(
            src_ref=cluster_send,
            dst_ref=cluster_recv.at[r - 1],
            send_sem=part_send_sem.at[r - 1],
            recv_sem=part_recv_sem.at[r - 1],
            device_id=(mates[r - 1],),
            device_id_type=MESH,
        )

    for r in range(1, 4):
        part_copy(r).start()

    def coef_copy(i, slot, dev):
        return pltpu.make_async_remote_copy(
            src_ref=x0.at[13],
            dst_ref=x0.at[slot],
            send_sem=coef_send_sem.at[i],
            recv_sem=coef_recv_sem.at[slot],
            device_id=(dev,),
            device_id_type=MESH,
        )

    for_each(coef_partners, lambda i, dev: coef_copy(i, 26 - i, dev).start())

    layer_ok = (side_z[0][1], None, side_z[1][1])
    spans = ((1, 2, None), (0, 1, side_x[0][1]), (3, 1, side_x[1][1]))

    def both(*flags):
        result = None
        for flag in flags:
            if flag is not None:
                result = flag if result is None else result & flag
        return result

    def panel_copy(source, target, leaves, index, dev):
        return pltpu.make_async_remote_copy(
            src_ref=pbuf.at[pl.ds(source, leaves)],
            dst_ref=pbuf.at[pl.ds(target, leaves)],
            send_sem=panel_send_sem.at[index],
            recv_sem=panel_recv_sem.at[index],
            device_id=(dev,),
            device_id_type=MESH,
        )

    def copy_z(d):
        return panel_copy(own_slot, 4 * (5 - 2 * d) + 1, 2, d, side_z[d][0])

    def copy_x(d, a):
        row = 4 * (3 + a)
        return panel_copy(row + 1 + d, row + 3 - 3 * d, 1, 2 + 3 * d + a, side_x[d][0])

    def copy_y(d, a, n):
        first, leaves, _ = spans[n]
        source = 4 * (3 + a) + first
        target = 4 * (3 * (2 - 2 * d) + a) + first
        return panel_copy(source, target, leaves, 8 + 9 * d + 3 * a + n, side_y[d][0])

    def panel_jobs():
        for d in range(2):
            yield side_z[d][1], copy_z(d)
        for d in range(2):
            for a in range(3):
                yield both(side_x[d][1], layer_ok[a]), copy_x(d, a)
        for d in range(2):
            for a in range(3):
                for n in range(3):
                    yield both(side_y[d][1], layer_ok[a], spans[n][2]), copy_y(d, a, n)

    def run_if(flag, action):
        if flag is None:
            action()
        else:
            pl.when(flag)(action)

    def start_x(a):
        for d in range(2):
            run_if(both(side_x[d][1], layer_ok[a]), copy_x(d, a).start)

    def start_y(a, n):
        for d in range(2):
            run_if(both(side_y[d][1], layer_ok[a], spans[n][2]), copy_y(d, a, n).start)

    for d in range(2):
        run_if(side_z[d][1], copy_z(d).start)
    start_x(1)
    start_y(1, 0)

    for r in range(1, 4):
        part_copy(r).wait_recv()
    total = cluster_send[...] + cluster_recv[0] + cluster_recv[1] + cluster_recv[2]
    x1_own[...] = total.astype(jnp.bfloat16)

    def clus_copy(i, slot, dev):
        return pltpu.make_async_remote_copy(
            src_ref=x1_own,
            dst_ref=x1.at[slot],
            send_sem=clus_send_sem.at[i],
            recv_sem=clus_recv_sem.at[slot],
            device_id=(dev,),
            device_id_type=MESH,
        )

    for_each(clusters, lambda i, dev: clus_copy(i, parent // 4, dev).start())

    load_raw.wait()
    split_levels(raw, turn, (m0, m1))
    for table in (m0, m1):
        for dx in (2, 3, 4):
            for dy in (2, 3, 4):
                first = 49 * dx + 7 * dy + 2
                table[pl.ds(first, 3)] = jnp.zeros((3, HALF, PAIR), jnp.bfloat16)

    for a, d in ((0, 1), (2, 0)):
        run_if(layer_ok[a], copy_z(d).wait_recv)
        start_x(a)
        start_y(a, 0)
    for a in (1, 0, 2):
        for n, d in ((1, 1), (2, 0)):
            run_if(both(spans[n][2], layer_ok[a]), copy_x(d, a).wait_recv)
            start_y(a, n)

    for_each(coef_partners, lambda i, dev: coef_copy(i, i, me).wait_recv())
    chunks = [list(range(first, min(first + 4, 27))) for first in range(0, 27, 4)]
    for t, chunk in enumerate(chunks):
        rows = x0[pl.ds(chunk[0], len(chunk))].reshape(len(chunk) * RANK, PAIR)
        xt[t, :, : len(chunk) * RANK] = rows.T
    lanes = lax.broadcasted_iota(jnp.int32, (COLS, PAIR), 1)
    base = 7 * gy + gz
    for tz in range(2):
        for ty in range(2):
            acc = jnp.zeros((PAIR, 2 * PAIR), jnp.float32)
            for t, chunk in enumerate(chunks):
                columns = []
                for tx in range(2):
                    column = []
                    for e in chunk:
                        ex, ey, ez = OFFSETS[e]
                        for h in range(2):
                            code = (
                                49 * (2 * ex + h - tx + 3)
                                + 7 * (2 * ey - ty + 3)
                                + (2 * ez - tz + 3)
                            )
                            column.append(m0[base + code])
                    columns.append(jnp.concatenate(column, axis=0))
                weights = jnp.concatenate(columns, axis=1)
                acc = acc + jnp.dot(
                    xt[t, :, : len(chunk) * RANK], weights, preferred_element_type=jnp.float32
                )
            first = acc[:COLS, :PAIR] + pltpu.roll(acc[COLS:, :PAIR], COLS, 1)
            second = pltpu.roll(acc[:COLS, PAIR:], COLS, 1) + acc[COLS:, PAIR:]
            sum_send[2 * tz + ty, :COLS, :] = jnp.where(lanes < COLS, first, second)

    for_each(clusters, lambda i, dev: clus_copy(i, i, me).wait_recv())
    acc = jnp.zeros((PAIR, PAIR), jnp.float32)
    for t in range(2):
        column = []
        for i in range(8 * t, 8 * t + 8):
            column.append(m1[cluster_base + clusters[i][2]])
        rows = x1[pl.ds(8 * t, 8)].reshape(8 * HALF, PAIR)
        acc = acc + jnp.dot(
            rows.T, jnp.concatenate(column, axis=0), preferred_element_type=jnp.float32
        )
    down = acc[:COLS] + pltpu.roll(acc[COLS:], COLS, 1)
    down = jnp.where(lanes[:HALF] < COLS, down[:HALF], pltpu.roll(down[HALF:], COLS, 1))
    for n in range(4):
        sum_send[n, COLS:, :] = down

    def sum_copy(r):
        return pltpu.make_async_remote_copy(
            src_ref=sum_send.at[(g + r) % 4],
            dst_ref=sum_recv.at[r - 1],
            send_sem=sum_send_sem.at[r - 1],
            recv_sem=sum_recv_sem.at[r - 1],
            device_id=(mates[r - 1],),
            device_id_type=MESH,
        )

    for r in range(1, 4):
        sum_copy(r).start()

    for d in range(2):
        for a in range(3):
            for n in range(3):
                run_if(
                    both(side_y[1 - d][1], layer_ok[a], spans[n][2]), copy_y(d, a, n).wait_recv
                )
    load_near.wait()
    load_list.wait()

    def slot_of(entry):
        lx = ((entry >> 0) & 1) + 2 * ((entry >> 3) & 1) + 4 * ((entry >> 6) & 1)
        ly = ((entry >> 1) & 1) + 2 * ((entry >> 4) & 1) + 4 * ((entry >> 7) & 1)
        lz = ((entry >> 2) & 1) + 2 * ((entry >> 5) & 1) + 4 * ((entry >> 8) & 1)
        slot = ((ly - y + 1) * 3 + lz - z + 1) * 4 + lx - 2 * bx + 1
        return jnp.where(entry < 0, ZERO_SLOT, jnp.clip(slot, 0, ZERO_SLOT))

    near_terms = []
    for h in range(2):
        acc = jnp.zeros((COLS, LEAF), jnp.float32)
        for k in range(NNEAR):
            acc = acc + jnp.dot(
                pbuf[slot_of(list_ref[h, k])], nbuf[h, k], preferred_element_type=jnp.float32
            )
        near_terms.append(acc)

    for r in range(1, 4):
        sum_copy(r).wait_recv()
    sums = sum_send[g] + sum_recv[0] + sum_recv[1] + sum_recv[2]
    down = jnp.concatenate([sums[COLS:, :COLS], sums[COLS:, COLS:]], axis=0).astype(jnp.bfloat16)
    for h in range(2):
        far_coef = sums[:COLS, COLS * h : COLS * (h + 1)] + lax.dot_general(
            down,
            transfer_vmem[h],
            (((1,), (1,)), ((), ())),
            preferred_element_type=jnp.float32,
        )
        far_term = jnp.dot(
            far_coef.astype(jnp.bfloat16), basis_vmem[h], preferred_element_type=jnp.float32
        )
        out_ref[h] = (near_terms[h] + far_term).astype(jnp.bfloat16)

    for r in range(1, 4):
        part_copy(r).wait_send()
        sum_copy(r).wait_send()

    for_each(coef_partners, lambda i, dev: coef_copy(i, 26 - i, dev).wait_send())
    for_each(clusters, lambda i, dev: clus_copy(i, parent // 4, dev).wait_send())
    for flag, copy in panel_jobs():
        run_if(flag, copy.wait_send)


def per_device(panels, basis, transfer, near_blocks, coupling, near_list):
    tables = coupling.reshape(2, SHIFTS, HALF, PAIR).transpose(1, 2, 0, 3)
    tables = tables.reshape(SHIFTS, RANK, PAIR)
    vmem = pl.BlockSpec(memory_space=pltpu.VMEM)
    hbm = pl.BlockSpec(memory_space=pltpu.HBM)
    dma = pltpu.SemaphoreType.DMA
    return pl.pallas_call(
        kernel,
        name="h2_product",
        out_shape=jax.ShapeDtypeStruct((2, COLS, LEAF), jnp.bfloat16),
        in_specs=[hbm] * 6,
        out_specs=vmem,
        scratch_shapes=[
            pltpu.VMEM((37, COLS, LEAF), jnp.bfloat16),
            pltpu.VMEM((2, NNEAR, LEAF, LEAF), jnp.bfloat16),
            pltpu.SMEM((2, NNEAR), jnp.int32),
            pltpu.VMEM((2, RANK, LEAF), jnp.bfloat16),
            pltpu.VMEM((2, RANK, RANK), jnp.bfloat16),
            pltpu.VMEM((SHIFTS, RANK, PAIR), jnp.bfloat16),
            pltpu.VMEM((SHIFTS, HALF, PAIR), jnp.bfloat16),
            pltpu.VMEM((SHIFTS, HALF, PAIR), jnp.bfloat16),
            pltpu.VMEM((27, RANK, PAIR), jnp.bfloat16),
            pltpu.VMEM((16, HALF, PAIR), jnp.bfloat16),
            pltpu.VMEM((HALF, PAIR), jnp.bfloat16),
            pltpu.VMEM((HALF, PAIR), jnp.float32),
            pltpu.VMEM((3, HALF, PAIR), jnp.float32),
            pltpu.VMEM((4, COLS + HALF, PAIR), jnp.float32),
            pltpu.VMEM((3, COLS + HALF, PAIR), jnp.float32),
            pltpu.VMEM((RANK, COLS), jnp.float32),
            pltpu.VMEM((GROUP * RANK, PAIR), jnp.float32),
            pltpu.VMEM((7, PAIR, 2 * PAIR), jnp.bfloat16),
            dma((6,)),
            dma((27,)),
            dma((27,)),
            dma((27,)),
            dma((27,)),
            dma((3,)),
            dma((3,)),
            dma((16,)),
            dma((16,)),
            dma((3,)),
            dma((3,)),
        ],
        compiler_params=pltpu.CompilerParams(
            collective_id=0, has_side_effects=True, vmem_limit_bytes=48 << 20
        ),
    )(*[pltpu.with_memory_space_constraint(a, pltpu.HBM) for a in (panels, basis, transfer, near_blocks, tables, near_list)])


def solution(mesh):
    return jax.shard_map(
        per_device,
        mesh=mesh,
        in_specs=(
            P(AXIS, None, None),
            P(AXIS, None, None),
            P(AXIS, None, None),
            P(AXIS, None, None, None),
            P(),
            P(AXIS, None),
        ),
        out_specs=P(AXIS, None, None),
        check_vma=False,
    )
```

```python
import jax
import jax.numpy as jnp
from jax import lax
from jax.experimental import pallas as pl
from jax.experimental.pallas import tpu as pltpu
from jax.sharding import PartitionSpec as P

MESH = pl.DeviceIdType.MESH
AXIS = "leaf"
LEAF = 256
RANK = 64
COLS = 64
NNEAR = 27
SHIFTS = 343
HALF = RANK // 2
PAIR = 2 * COLS
ZERO_SLOT = 36
GROUP = 7


def bit(value, k):
    return (value // (1 << k)) % 2


def device_position(dev):
    bx = bit(dev, 2) + 2 * bit(dev, 5)
    y = bit(dev, 0) + 2 * bit(dev, 3) + 4 * bit(dev, 6)
    z = bit(dev, 1) + 2 * bit(dev, 4) + 4 * bit(dev, 7)
    return bx, y, z


def cluster_position(p):
    px = bit(p, 0) + 2 * bit(p, 3)
    py = bit(p, 1) + 2 * bit(p, 4)
    pz = bit(p, 2) + 2 * bit(p, 5)
    return px, py, pz


OFFSETS = [(a, b, c) for a in (-1, 0, 1) for b in (-1, 0, 1) for c in (-1, 0, 1)]
CENTRE = 13


def split_rows(scratch, value):
    scratch[...] = value
    even = scratch[pl.ds(0, HALF, stride=2), :]
    odd = scratch[pl.ds(1, HALF, stride=2), :]
    return jnp.concatenate([even, odd], axis=1)


def split_levels(raw, turn, tables):
    group = turn.shape[0] // RANK

    def split(i, carry):
        first = i * group
        turn[...] = raw[pl.ds(first, group)].reshape(group * RANK, PAIR).astype(jnp.float32)
        for level, table in enumerate(tables):
            rows = turn[pl.ds(level, group * HALF, stride=2), :]
            table[pl.ds(first, group)] = rows.astype(jnp.bfloat16).reshape(group, HALF, PAIR)
        return carry

    lax.fori_loop(0, SHIFTS // group, split, 0)


def kernel(
    panels_ref,
    basis_ref,
    transfer_ref,
    near_ref,
    coupling_ref,
    list_hbm,
    out_ref,
    pbuf,
    nbuf,
    list_ref,
    basis_vmem,
    transfer_vmem,
    raw,
    m0,
    m1,
    x0,
    x1,
    x1_own,
    cluster_send,
    cluster_recv,
    sum_send,
    sum_recv,
    tmp,
    turn,
    xt,
    load_sem,
    panel_send_sem,
    panel_recv_sem,
    coef_send_sem,
    coef_recv_sem,
    part_send_sem,
    part_recv_sem,
    clus_send_sem,
    clus_recv_sem,
    sum_send_sem,
    sum_recv_sem,
):
    me = lax.axis_index(AXIS)
    g = me % 4
    gy = me % 2
    gz = (me // 2) % 2
    parent = me // 4
    bx, y, z = device_position(me)
    px, py, pz = cluster_position(parent)
    own_slot = 17

    load_panels = pltpu.make_async_copy(panels_ref, pbuf.at[pl.ds(own_slot, 2)], load_sem.at[0])
    load_panels.start()
    load_basis = pltpu.make_async_copy(basis_ref, basis_vmem, load_sem.at[1])
    load_basis.start()
    load_transfer = pltpu.make_async_copy(transfer_ref, transfer_vmem, load_sem.at[2])
    load_transfer.start()
    load_list = pltpu.make_async_copy(list_hbm, list_ref, load_sem.at[5])
    load_list.start()
    load_raw = pltpu.make_async_copy(coupling_ref, raw, load_sem.at[3])
    load_raw.start()
    load_near = pltpu.make_async_copy(near_ref, nbuf, load_sem.at[4])
    load_near.start()

    x0[...] = jnp.zeros_like(x0)
    x1[...] = jnp.zeros_like(x1)
    pbuf[ZERO_SLOT] = jnp.zeros((COLS, LEAF), jnp.bfloat16)

    def ones(flags):
        return sum(jnp.where(flag, 1, 0) for flag in flags)

    def place_of(position):
        tx, ty, tz = position
        share_x = 4 * bit(tx, 0) + 32 * bit(tx, 1)
        share_y = bit(ty, 0) + 8 * bit(ty, 1) + 64 * bit(ty, 2)
        share_z = 2 * bit(tz, 0) + 16 * bit(tz, 1) + 128 * bit(tz, 2)
        return share_x + share_y + share_z

    side_x = [(place_of((bx + d, y, z)), ok) for d, ok in ((-1, bx > 0), (1, bx < 3))]
    side_y = [(place_of((bx, y + d, z)), ok) for d, ok in ((-1, y > 0), (1, y < 7))]
    side_z = [(place_of((bx, y, z + d)), ok) for d, ok in ((-1, z > 0), (1, z < 7))]
    panel_count = ones([ok for _, ok in side_x + side_y + side_z])
    def device_of(tx, ty, tz):
        share_x = 4 * bit(tx, 0) + 32 * bit(tx, 1)
        share_y = 8 * bit(ty, 0) + 64 * bit(ty, 1)
        share_z = 16 * bit(tz, 0) + 128 * bit(tz, 1)
        return share_x + share_y + share_z + g

    coef_x = [(device_of(px + d, py, pz), ok) for d, ok in ((-1, px > 0), (1, px < 3))]
    coef_y = [(device_of(px, py + d, pz), ok) for d, ok in ((-1, py > 0), (1, py < 3))]
    coef_z = [(device_of(px, py, pz + d), ok) for d, ok in ((-1, pz > 0), (1, pz < 3))]
    coef_count = ones([ok for _, ok in coef_x + coef_y + coef_z])

    def close(q, p):
        return (q - p < 2) & (p - q < 2)

    near_x = [close(gy + 2 * k, px) for k in range(2)]
    near_y = [close(gz + 2 * k, py) for k in range(2)]
    near_z = [close(k, pz) for k in range(4)]
    clusters = []
    for i in range(16):
        kx, ky, kz = (i // 2) % 2, (i // 4) % 2, i % 2 + 2 * (i // 8)
        near = near_x[kx] & near_y[ky] & near_z[kz]
        dev = 16 * i + 4 * g + parent % 4
        clusters.append((dev, jnp.logical_not(near), 98 * kx + 14 * ky + kz))
    cluster_base = 49 * (gy - px + 3) + 7 * (gz - py + 3) + 3 - pz

    cluster_count = 16 - ones(near_x) * ones(near_y) * ones(near_z)
    mates = [4 * parent + (g + r) % 4 for r in range(1, 4)]

    def for_each(partners, action):
        for i, partner in enumerate(partners):
            if partner[1] is None:
                continue

            @pl.when(partner[1])
            def _():
                action(i, partner[0])

    barrier = pltpu.get_barrier_semaphore()

    def greet(i, dev):
        pl.semaphore_signal(barrier, inc=1, device_id=(dev,), device_id_type=MESH)

    for dev in mates:
        greet(0, dev)
    for_each(side_x + side_y + side_z, greet)
    for_each(coef_x + coef_y + coef_z, greet)
    for_each(clusters, greet)
    count = panel_count + coef_count + cluster_count + 3

    load_panels.wait()
    load_basis.wait()
    load_transfer.wait()
    part = jnp.zeros((RANK, COLS), jnp.float32)
    for h in range(2):
        coef = lax.dot_general(
            basis_vmem[h],
            pbuf[own_slot + h],
            (((1,), (1,)), ((), ())),
            preferred_element_type=jnp.float32,
        )
        x0[13, pl.ds(HALF * h, HALF), :] = split_rows(tmp, coef).astype(jnp.bfloat16)
        part = part + lax.dot_general(
            transfer_vmem[h],
            coef.astype(jnp.bfloat16),
            (((0,), (0,)), ((), ())),
            preferred_element_type=jnp.float32,
        )
    cluster_send[...] = split_rows(tmp, part)

    pl.semaphore_wait(barrier, count)

    def part_copy(r):
        return pltpu.make_async_remote_copy(
            src_ref=cluster_send,
            dst_ref=cluster_recv.at[r - 1],
            send_sem=part_send_sem.at[r - 1],
            recv_sem=part_recv_sem.at[r - 1],
            device_id=(mates[r - 1],),
            device_id_type=MESH,
        )

    for r in range(1, 4):
        part_copy(r).start()

    layer_ok = (side_z[0][1], None, side_z[1][1])
    spans = ((1, 2, None), (0, 1, side_x[0][1]), (3, 1, side_x[1][1]))

    def both(*flags):
        result = None
        for flag in flags:
            if flag is not None:
                result = flag if result is None else result & flag
        return result

    def run_if(flag, action):
        if flag is None:
            action()
        else:
            pl.when(flag)(action)

    def panel_copy(source, target, leaves, index, dev):
        return pltpu.make_async_remote_copy(
            src_ref=pbuf.at[pl.ds(source, leaves)],
            dst_ref=pbuf.at[pl.ds(target, leaves)],
            send_sem=panel_send_sem.at[index],
            recv_sem=panel_recv_sem.at[index],
            device_id=(dev,),
            device_id_type=MESH,
        )

    def coef_copy(source, target, index, dev):
        return pltpu.make_async_remote_copy(
            src_ref=x0.at[source],
            dst_ref=x0.at[target],
            send_sem=coef_send_sem.at[index],
            recv_sem=coef_recv_sem.at[index],
            device_id=(dev,),
            device_id_type=MESH,
        )

    coef_layers = (coef_z[0][1], None, coef_z[1][1])
    coef_sides = ((0, None), (-1, coef_y[0][1]), (1, coef_y[1][1]))

    def coef_to_z(d):
        return coef_z[d][1], coef_copy(CENTRE, CENTRE + 1 - 2 * d, d, coef_z[d][0])

    def coef_to_y(d, a):
        flag = both(coef_y[d][1], coef_layers[a])
        return flag, coef_copy(12 + a, 15 - 6 * d + a, 2 + 3 * d + a, coef_y[d][0])

    def coef_to_x(d, a, n):
        ey, ok = coef_sides[n]
        flag = both(coef_x[d][1], coef_layers[a], ok)
        source = 12 + 3 * ey + a
        return flag, coef_copy(
            source, source + 9 - 18 * d, 8 + 9 * d + 3 * a + n, coef_x[d][0]
        )

    def start(jobs):
        for flag, copy in jobs:
            run_if(flag, copy.start)

    def copy_z(d):
        return panel_copy(own_slot, 4 * (5 - 2 * d) + 1, 2, d, side_z[d][0])

    def copy_x(d, a):
        row = 4 * (3 + a)
        return panel_copy(row + 1 + d, row + 3 - 3 * d, 1, 2 + 3 * d + a, side_x[d][0])

    def copy_y(d, a, n):
        first, leaves, _ = spans[n]
        source = 4 * (3 + a) + first
        target = 4 * (3 * (2 - 2 * d) + a) + first
        return panel_copy(source, target, leaves, 8 + 9 * d + 3 * a + n, side_y[d][0])

    def panel_jobs():
        for d in range(2):
            yield side_z[d][1], copy_z(d)
        for d in range(2):
            for a in range(3):
                yield both(side_x[d][1], layer_ok[a]), copy_x(d, a)
        for d in range(2):
            for a in range(3):
                for n in range(3):
                    yield both(side_y[d][1], layer_ok[a], spans[n][2]), copy_y(d, a, n)

    def start_x(a):
        for d in range(2):
            run_if(both(side_x[d][1], layer_ok[a]), copy_x(d, a).start)

    def start_y(a, n):
        for d in range(2):
            run_if(both(side_y[d][1], layer_ok[a], spans[n][2]), copy_y(d, a, n).start)

    start([coef_to_z(d) for d in range(2)])
    for d in range(2):
        run_if(side_z[d][1], copy_z(d).start)
    start([coef_to_y(d, 1) for d in range(2)])
    start_x(1)
    start([coef_to_x(d, 1, 0) for d in range(2)])
    start_y(1, 0)

    for r in range(1, 4):
        part_copy(r).wait_recv()
    total = cluster_send[...] + cluster_recv[0] + cluster_recv[1] + cluster_recv[2]
    x1_own[...] = total.astype(jnp.bfloat16)

    def clus_copy(i, slot, dev):
        return pltpu.make_async_remote_copy(
            src_ref=x1_own,
            dst_ref=x1.at[slot],
            send_sem=clus_send_sem.at[i],
            recv_sem=clus_recv_sem.at[slot],
            device_id=(dev,),
            device_id_type=MESH,
        )

    for_each(clusters, lambda i, dev: clus_copy(i, parent // 4, dev).start())

    load_raw.wait()
    split_levels(raw, turn, (m0, m1))
    for table in (m0, m1):
        for dx in (2, 3, 4):
            for dy in (2, 3, 4):
                first = 49 * dx + 7 * dy + 2
                table[pl.ds(first, 3)] = jnp.zeros((3, HALF, PAIR), jnp.bfloat16)

    for a, d in ((0, 1), (2, 0)):
        run_if(coef_layers[a], coef_to_z(d)[1].wait_recv)
        start([coef_to_y(e, a) for e in range(2)])
        start([coef_to_x(e, a, 0) for e in range(2)])
    for a, d in ((0, 1), (2, 0)):
        run_if(layer_ok[a], copy_z(d).wait_recv)
        start_x(a)
        start_y(a, 0)
    for a in (1, 0, 2):
        for n, d in ((1, 1), (2, 0)):
            run_if(both(coef_sides[n][1], coef_layers[a]), coef_to_y(d, a)[1].wait_recv)
            start([coef_to_x(e, a, n) for e in range(2)])
    for a in (1, 0, 2):
        for n, d in ((1, 1), (2, 0)):
            run_if(both(spans[n][2], layer_ok[a]), copy_x(d, a).wait_recv)
            start_y(a, n)

    for d in range(2):
        for a in range(3):
            for n in range(3):
                flag = both(coef_x[1 - d][1], coef_layers[a], coef_sides[n][1])
                run_if(flag, coef_to_x(d, a, n)[1].wait_recv)
    chunks = [list(range(first, min(first + 4, 27))) for first in range(0, 27, 4)]
    for t, chunk in enumerate(chunks):
        rows = x0[pl.ds(chunk[0], len(chunk))].reshape(len(chunk) * RANK, PAIR)
        xt[t, :, : len(chunk) * RANK] = rows.T
    lanes = lax.broadcasted_iota(jnp.int32, (COLS, PAIR), 1)
    base = 7 * gy + gz
    for tz in range(2):
        for ty in range(2):
            acc = jnp.zeros((PAIR, 2 * PAIR), jnp.float32)
            for t, chunk in enumerate(chunks):
                columns = []
                for tx in range(2):
                    column = []
                    for e in chunk:
                        ex, ey, ez = OFFSETS[e]
                        for h in range(2):
                            code = (
                                49 * (2 * ex + h - tx + 3)
                                + 7 * (2 * ey - ty + 3)
                                + (2 * ez - tz + 3)
                            )
                            column.append(m0[base + code])
                    columns.append(jnp.concatenate(column, axis=0))
                weights = jnp.concatenate(columns, axis=1)
                acc = acc + jnp.dot(
                    xt[t, :, : len(chunk) * RANK], weights, preferred_element_type=jnp.float32
                )
            first = acc[:COLS, :PAIR] + pltpu.roll(acc[COLS:, :PAIR], COLS, 1)
            second = pltpu.roll(acc[:COLS, PAIR:], COLS, 1) + acc[COLS:, PAIR:]
            sum_send[2 * tz + ty, :COLS, :] = jnp.where(lanes < COLS, first, second)

    for_each(clusters, lambda i, dev: clus_copy(i, i, me).wait_recv())
    acc = jnp.zeros((PAIR, PAIR), jnp.float32)
    for t in range(2):
        column = []
        for i in range(8 * t, 8 * t + 8):
            column.append(m1[cluster_base + clusters[i][2]])
        rows = x1[pl.ds(8 * t, 8)].reshape(8 * HALF, PAIR)
        acc = acc + jnp.dot(
            rows.T, jnp.concatenate(column, axis=0), preferred_element_type=jnp.float32
        )
    down = acc[:COLS] + pltpu.roll(acc[COLS:], COLS, 1)
    down = jnp.where(lanes[:HALF] < COLS, down[:HALF], pltpu.roll(down[HALF:], COLS, 1))
    for n in range(4):
        sum_send[n, COLS:, :] = down

    def sum_copy(r):
        return pltpu.make_async_remote_copy(
            src_ref=sum_send.at[(g + r) % 4],
            dst_ref=sum_recv.at[r - 1],
            send_sem=sum_send_sem.at[r - 1],
            recv_sem=sum_recv_sem.at[r - 1],
            device_id=(mates[r - 1],),
            device_id_type=MESH,
        )

    for r in range(1, 4):
        sum_copy(r).start()

    for d in range(2):
        for a in range(3):
            for n in range(3):
                run_if(
                    both(side_y[1 - d][1], layer_ok[a], spans[n][2]), copy_y(d, a, n).wait_recv
                )
    load_near.wait()
    load_list.wait()

    def slot_of(entry):
        lx = ((entry >> 0) & 1) + 2 * ((entry >> 3) & 1) + 4 * ((entry >> 6) & 1)
        ly = ((entry >> 1) & 1) + 2 * ((entry >> 4) & 1) + 4 * ((entry >> 7) & 1)
        lz = ((entry >> 2) & 1) + 2 * ((entry >> 5) & 1) + 4 * ((entry >> 8) & 1)
        slot = ((ly - y + 1) * 3 + lz - z + 1) * 4 + lx - 2 * bx + 1
        return jnp.where(entry < 0, ZERO_SLOT, jnp.clip(slot, 0, ZERO_SLOT))

    near_terms = []
    for h in range(2):
        acc = jnp.zeros((COLS, LEAF), jnp.float32)
        for k in range(NNEAR):
            acc = acc + jnp.dot(
                pbuf[slot_of(list_ref[h, k])], nbuf[h, k], preferred_element_type=jnp.float32
            )
        near_terms.append(acc)

    for r in range(1, 4):
        sum_copy(r).wait_recv()
    sums = sum_send[g] + sum_recv[0] + sum_recv[1] + sum_recv[2]
    down = jnp.concatenate([sums[COLS:, :COLS], sums[COLS:, COLS:]], axis=0).astype(jnp.bfloat16)
    for h in range(2):
        far_coef = sums[:COLS, COLS * h : COLS * (h + 1)] + lax.dot_general(
            down,
            transfer_vmem[h],
            (((1,), (1,)), ((), ())),
            preferred_element_type=jnp.float32,
        )
        far_term = jnp.dot(
            far_coef.astype(jnp.bfloat16), basis_vmem[h], preferred_element_type=jnp.float32
        )
        out_ref[h] = (near_terms[h] + far_term).astype(jnp.bfloat16)

    for r in range(1, 4):
        part_copy(r).wait_send()
        sum_copy(r).wait_send()

    coef_jobs = [coef_to_z(d) for d in range(2)]
    coef_jobs += [coef_to_y(d, a) for d in range(2) for a in range(3)]
    coef_jobs += [coef_to_x(d, a, n) for d in range(2) for a in range(3) for n in range(3)]
    for flag, copy in coef_jobs:
        run_if(flag, copy.wait_send)
    for_each(clusters, lambda i, dev: clus_copy(i, parent // 4, dev).wait_send())
    for flag, copy in panel_jobs():
        run_if(flag, copy.wait_send)


def per_device(panels, basis, transfer, near_blocks, coupling, near_list):
    tables = coupling.reshape(2, SHIFTS, HALF, PAIR).transpose(1, 2, 0, 3)
    tables = tables.reshape(SHIFTS, RANK, PAIR)
    vmem = pl.BlockSpec(memory_space=pltpu.VMEM)
    hbm = pl.BlockSpec(memory_space=pltpu.HBM)
    dma = pltpu.SemaphoreType.DMA
    return pl.pallas_call(
        kernel,
        name="h2_product",
        out_shape=jax.ShapeDtypeStruct((2, COLS, LEAF), jnp.bfloat16),
        in_specs=[hbm] * 6,
        out_specs=vmem,
        scratch_shapes=[
            pltpu.VMEM((37, COLS, LEAF), jnp.bfloat16),
            pltpu.VMEM((2, NNEAR, LEAF, LEAF), jnp.bfloat16),
            pltpu.SMEM((2, NNEAR), jnp.int32),
            pltpu.VMEM((2, RANK, LEAF), jnp.bfloat16),
            pltpu.VMEM((2, RANK, RANK), jnp.bfloat16),
            pltpu.VMEM((SHIFTS, RANK, PAIR), jnp.bfloat16),
            pltpu.VMEM((SHIFTS, HALF, PAIR), jnp.bfloat16),
            pltpu.VMEM((SHIFTS, HALF, PAIR), jnp.bfloat16),
            pltpu.VMEM((27, RANK, PAIR), jnp.bfloat16),
            pltpu.VMEM((16, HALF, PAIR), jnp.bfloat16),
            pltpu.VMEM((HALF, PAIR), jnp.bfloat16),
            pltpu.VMEM((HALF, PAIR), jnp.float32),
            pltpu.VMEM((3, HALF, PAIR), jnp.float32),
            pltpu.VMEM((4, COLS + HALF, PAIR), jnp.float32),
            pltpu.VMEM((3, COLS + HALF, PAIR), jnp.float32),
            pltpu.VMEM((RANK, COLS), jnp.float32),
            pltpu.VMEM((GROUP * RANK, PAIR), jnp.float32),
            pltpu.VMEM((7, PAIR, 2 * PAIR), jnp.bfloat16),
            dma((6,)),
            dma((27,)),
            dma((27,)),
            dma((27,)),
            dma((27,)),
            dma((3,)),
            dma((3,)),
            dma((16,)),
            dma((16,)),
            dma((3,)),
            dma((3,)),
        ],
        compiler_params=pltpu.CompilerParams(
            collective_id=0, has_side_effects=True, vmem_limit_bytes=48 << 20
        ),
    )(*[pltpu.with_memory_space_constraint(a, pltpu.HBM) for a in (panels, basis, transfer, near_blocks, tables, near_list)])


def solution(mesh):
    return jax.shard_map(
        per_device,
        mesh=mesh,
        in_specs=(
            P(AXIS, None, None),
            P(AXIS, None, None),
            P(AXIS, None, None),
            P(AXIS, None, None, None),
            P(),
            P(AXIS, None),
        ),
        out_specs=P(AXIS, None, None),
        check_vma=False,
    )
```

```python
import jax
import jax.numpy as jnp
from jax import lax
from jax.experimental import pallas as pl
from jax.experimental.pallas import tpu as pltpu
from jax.sharding import PartitionSpec as P

MESH = pl.DeviceIdType.MESH
AXIS = "leaf"
LEAF = 256
RANK = 64
COLS = 64
NNEAR = 27
SHIFTS = 343
HALF = RANK // 2
PAIR = 2 * COLS
ZERO_SLOT = 36
GROUP = 7


def bit(value, k):
    return (value // (1 << k)) % 2


def device_position(dev):
    bx = bit(dev, 2) + 2 * bit(dev, 5)
    y = bit(dev, 0) + 2 * bit(dev, 3) + 4 * bit(dev, 6)
    z = bit(dev, 1) + 2 * bit(dev, 4) + 4 * bit(dev, 7)
    return bx, y, z


def cluster_position(p):
    px = bit(p, 0) + 2 * bit(p, 3)
    py = bit(p, 1) + 2 * bit(p, 4)
    pz = bit(p, 2) + 2 * bit(p, 5)
    return px, py, pz


OFFSETS = [(a, b, c) for a in (-1, 0, 1) for b in (-1, 0, 1) for c in (-1, 0, 1)]
CENTRE = 13


def split_rows(scratch, value):
    scratch[...] = value
    even = scratch[pl.ds(0, HALF, stride=2), :]
    odd = scratch[pl.ds(1, HALF, stride=2), :]
    return jnp.concatenate([even, odd], axis=1)


def split_levels(raw, turn, tables):
    group = turn.shape[0] // RANK

    def split(i, carry):
        first = i * group
        turn[...] = raw[pl.ds(first, group)].reshape(group * RANK, PAIR).astype(jnp.float32)
        for level, table in enumerate(tables):
            rows = turn[pl.ds(level, group * HALF, stride=2), :]
            table[pl.ds(first, group)] = rows.astype(jnp.bfloat16).reshape(group, HALF, PAIR)
        return carry

    lax.fori_loop(0, SHIFTS // group, split, 0)


def kernel(
    panels_ref,
    basis_ref,
    transfer_ref,
    near_ref,
    coupling_ref,
    list_hbm,
    out_ref,
    pbuf,
    nbuf,
    list_ref,
    basis_vmem,
    transfer_vmem,
    raw,
    m0,
    m1,
    x0,
    x1,
    x1_own,
    cluster_send,
    cluster_recv,
    sum_send,
    sum_recv,
    tmp,
    turn,
    xt,
    load_sem,
    panel_send_sem,
    panel_recv_sem,
    coef_send_sem,
    coef_recv_sem,
    part_send_sem,
    part_recv_sem,
    clus_send_sem,
    clus_recv_sem,
    sum_send_sem,
    sum_recv_sem,
):
    me = lax.axis_index(AXIS)
    g = me % 4
    gy = me % 2
    gz = (me // 2) % 2
    parent = me // 4
    bx, y, z = device_position(me)
    px, py, pz = cluster_position(parent)
    own_slot = 17

    load_panels = pltpu.make_async_copy(panels_ref, pbuf.at[pl.ds(own_slot, 2)], load_sem.at[0])
    load_panels.start()
    load_basis = pltpu.make_async_copy(basis_ref, basis_vmem, load_sem.at[1])
    load_basis.start()
    load_transfer = pltpu.make_async_copy(transfer_ref, transfer_vmem, load_sem.at[2])
    load_transfer.start()
    load_list = pltpu.make_async_copy(list_hbm, list_ref, load_sem.at[5])
    load_list.start()
    load_raw = pltpu.make_async_copy(coupling_ref, raw, load_sem.at[3])
    load_raw.start()
    load_near = pltpu.make_async_copy(near_ref, nbuf, load_sem.at[4])
    load_near.start()

    x0[...] = jnp.zeros_like(x0)
    x1[...] = jnp.zeros_like(x1)
    pbuf[ZERO_SLOT] = jnp.zeros((COLS, LEAF), jnp.bfloat16)

    def ones(flags):
        return sum(jnp.where(flag, 1, 0) for flag in flags)

    def place_of(position):
        tx, ty, tz = position
        share_x = 4 * bit(tx, 0) + 32 * bit(tx, 1)
        share_y = bit(ty, 0) + 8 * bit(ty, 1) + 64 * bit(ty, 2)
        share_z = 2 * bit(tz, 0) + 16 * bit(tz, 1) + 128 * bit(tz, 2)
        return share_x + share_y + share_z

    side_x = [(place_of((bx + d, y, z)), ok) for d, ok in ((-1, bx > 0), (1, bx < 3))]
    side_y = [(place_of((bx, y + d, z)), ok) for d, ok in ((-1, y > 0), (1, y < 7))]
    side_z = [(place_of((bx, y, z + d)), ok) for d, ok in ((-1, z > 0), (1, z < 7))]
    panel_count = ones([ok for _, ok in side_x + side_y + side_z])
    def device_of(tx, ty, tz):
        share_x = 4 * bit(tx, 0) + 32 * bit(tx, 1)
        share_y = 8 * bit(ty, 0) + 64 * bit(ty, 1)
        share_z = 16 * bit(tz, 0) + 128 * bit(tz, 1)
        return share_x + share_y + share_z + g

    coef_x = [(device_of(px + d, py, pz), ok) for d, ok in ((-1, px > 0), (1, px < 3))]
    coef_y = [(device_of(px, py + d, pz), ok) for d, ok in ((-1, py > 0), (1, py < 3))]
    coef_z = [(device_of(px, py, pz + d), ok) for d, ok in ((-1, pz > 0), (1, pz < 3))]
    coef_count = ones([ok for _, ok in coef_x + coef_y + coef_z])

    def close(q, p):
        return (q - p < 2) & (p - q < 2)

    near_x = [close(gy + 2 * k, px) for k in range(2)]
    near_y = [close(gz + 2 * k, py) for k in range(2)]
    near_z = [close(k, pz) for k in range(4)]
    clusters = []
    for i in range(16):
        kx, ky, kz = (i // 2) % 2, (i // 4) % 2, i % 2 + 2 * (i // 8)
        near = near_x[kx] & near_y[ky] & near_z[kz]
        dev = 16 * i + 4 * g + parent % 4
        clusters.append((dev, jnp.logical_not(near), 98 * kx + 14 * ky + kz))
    cluster_base = 49 * (gy - px + 3) + 7 * (gz - py + 3) + 3 - pz

    cluster_count = 16 - ones(near_x) * ones(near_y) * ones(near_z)
    mates = [4 * parent + (g + r) % 4 for r in range(1, 4)]

    def for_each(partners, action):
        for i, partner in enumerate(partners):
            if partner[1] is None:
                continue

            @pl.when(partner[1])
            def _():
                action(i, partner[0])

    barrier = pltpu.get_barrier_semaphore()

    def greet(i, dev):
        pl.semaphore_signal(barrier, inc=1, device_id=(dev,), device_id_type=MESH)

    for dev in mates:
        greet(0, dev)
    for_each(side_x + side_y + side_z, greet)
    for_each(coef_x + coef_y + coef_z, greet)
    for_each(clusters, greet)
    count = panel_count + coef_count + cluster_count + 3

    load_panels.wait()
    load_basis.wait()
    load_transfer.wait()
    part = jnp.zeros((RANK, COLS), jnp.float32)
    for h in range(2):
        coef = lax.dot_general(
            basis_vmem[h],
            pbuf[own_slot + h],
            (((1,), (1,)), ((), ())),
            preferred_element_type=jnp.float32,
        )
        x0[13, pl.ds(HALF * h, HALF), :] = split_rows(tmp, coef).astype(jnp.bfloat16)
        part = part + lax.dot_general(
            transfer_vmem[h],
            coef.astype(jnp.bfloat16),
            (((0,), (0,)), ((), ())),
            preferred_element_type=jnp.float32,
        )
    cluster_send[...] = split_rows(tmp, part)

    def prepare_tables():
        load_raw.wait()
        split_levels(raw, turn, (m0, m1))
        for table in (m0, m1):
            for dx in (2, 3, 4):
                for dy in (2, 3, 4):
                    first = 49 * dx + 7 * dy + 2
                    table[pl.ds(first, 3)] = jnp.zeros((3, HALF, PAIR), jnp.bfloat16)


    pl.when(z < 4)(prepare_tables)

    pl.semaphore_wait(barrier, count)

    def part_copy(r):
        return pltpu.make_async_remote_copy(
            src_ref=cluster_send,
            dst_ref=cluster_recv.at[r - 1],
            send_sem=part_send_sem.at[r - 1],
            recv_sem=part_recv_sem.at[r - 1],
            device_id=(mates[r - 1],),
            device_id_type=MESH,
        )

    for r in range(1, 4):
        part_copy(r).start()

    layer_ok = (side_z[0][1], None, side_z[1][1])
    spans = ((1, 2, None), (0, 1, side_x[0][1]), (3, 1, side_x[1][1]))

    def both(*flags):
        result = None
        for flag in flags:
            if flag is not None:
                result = flag if result is None else result & flag
        return result

    def run_if(flag, action):
        if flag is None:
            action()
        else:
            pl.when(flag)(action)

    def panel_copy(source, target, leaves, index, dev):
        return pltpu.make_async_remote_copy(
            src_ref=pbuf.at[pl.ds(source, leaves)],
            dst_ref=pbuf.at[pl.ds(target, leaves)],
            send_sem=panel_send_sem.at[index],
            recv_sem=panel_recv_sem.at[index],
            device_id=(dev,),
            device_id_type=MESH,
        )

    def coef_copy(source, target, index, dev):
        return pltpu.make_async_remote_copy(
            src_ref=x0.at[source],
            dst_ref=x0.at[target],
            send_sem=coef_send_sem.at[index],
            recv_sem=coef_recv_sem.at[index],
            device_id=(dev,),
            device_id_type=MESH,
        )

    coef_layers = (coef_z[0][1], None, coef_z[1][1])
    coef_sides = ((0, None), (-1, coef_y[0][1]), (1, coef_y[1][1]))

    def coef_to_z(d):
        return coef_z[d][1], coef_copy(CENTRE, CENTRE + 1 - 2 * d, d, coef_z[d][0])

    def coef_to_y(d, a):
        flag = both(coef_y[d][1], coef_layers[a])
        return flag, coef_copy(12 + a, 15 - 6 * d + a, 2 + 3 * d + a, coef_y[d][0])

    def coef_to_x(d, a, n):
        ey, ok = coef_sides[n]
        flag = both(coef_x[d][1], coef_layers[a], ok)
        source = 12 + 3 * ey + a
        return flag, coef_copy(
            source, source + 9 - 18 * d, 8 + 9 * d + 3 * a + n, coef_x[d][0]
        )

    def start(jobs):
        for flag, copy in jobs:
            run_if(flag, copy.start)

    def copy_z(d):
        return panel_copy(own_slot, 4 * (5 - 2 * d) + 1, 2, d, side_z[d][0])

    def copy_x(d, a):
        row = 4 * (3 + a)
        return panel_copy(row + 1 + d, row + 3 - 3 * d, 1, 2 + 3 * d + a, side_x[d][0])

    def copy_y(d, a, n):
        first, leaves, _ = spans[n]
        source = 4 * (3 + a) + first
        target = 4 * (3 * (2 - 2 * d) + a) + first
        return panel_copy(source, target, leaves, 8 + 9 * d + 3 * a + n, side_y[d][0])

    def panel_jobs():
        for d in range(2):
            yield side_z[d][1], copy_z(d)
        for d in range(2):
            for a in range(3):
                yield both(side_x[d][1], layer_ok[a]), copy_x(d, a)
        for d in range(2):
            for a in range(3):
                for n in range(3):
                    yield both(side_y[d][1], layer_ok[a], spans[n][2]), copy_y(d, a, n)

    def start_x(a):
        for d in range(2):
            run_if(both(side_x[d][1], layer_ok[a]), copy_x(d, a).start)

    def start_y(a, n):
        for d in range(2):
            run_if(both(side_y[d][1], layer_ok[a], spans[n][2]), copy_y(d, a, n).start)

    start([coef_to_z(d) for d in range(2)])
    for d in range(2):
        run_if(side_z[d][1], copy_z(d).start)
    start([coef_to_y(d, 1) for d in range(2)])
    start_x(1)
    start([coef_to_x(d, 1, 0) for d in range(2)])
    start_y(1, 0)

    for r in range(1, 4):
        part_copy(r).wait_recv()
    total = cluster_send[...] + cluster_recv[0] + cluster_recv[1] + cluster_recv[2]
    x1_own[...] = total.astype(jnp.bfloat16)

    def clus_copy(i, slot, dev):
        return pltpu.make_async_remote_copy(
            src_ref=x1_own,
            dst_ref=x1.at[slot],
            send_sem=clus_send_sem.at[i],
            recv_sem=clus_recv_sem.at[slot],
            device_id=(dev,),
            device_id_type=MESH,
        )

    for_each(clusters, lambda i, dev: clus_copy(i, parent // 4, dev).start())

    pl.when(z >= 4)(prepare_tables)

    for a, d in ((0, 1), (2, 0)):
        run_if(coef_layers[a], coef_to_z(d)[1].wait_recv)
        start([coef_to_y(e, a) for e in range(2)])
        start([coef_to_x(e, a, 0) for e in range(2)])
    for a, d in ((0, 1), (2, 0)):
        run_if(layer_ok[a], copy_z(d).wait_recv)
        start_x(a)
        start_y(a, 0)
    for a in (1, 0, 2):
        for n, d in ((1, 1), (2, 0)):
            run_if(both(coef_sides[n][1], coef_layers[a]), coef_to_y(d, a)[1].wait_recv)
            start([coef_to_x(e, a, n) for e in range(2)])
    for a in (1, 0, 2):
        for n, d in ((1, 1), (2, 0)):
            run_if(both(spans[n][2], layer_ok[a]), copy_x(d, a).wait_recv)
            start_y(a, n)

    for d in range(2):
        for a in range(3):
            for n in range(3):
                flag = both(coef_x[1 - d][1], coef_layers[a], coef_sides[n][1])
                run_if(flag, coef_to_x(d, a, n)[1].wait_recv)
    chunks = [list(range(first, min(first + 4, 27))) for first in range(0, 27, 4)]
    for t, chunk in enumerate(chunks):
        rows = x0[pl.ds(chunk[0], len(chunk))].reshape(len(chunk) * RANK, PAIR)
        xt[t, :, : len(chunk) * RANK] = rows.T
    lanes = lax.broadcasted_iota(jnp.int32, (COLS, PAIR), 1)
    base = 7 * gy + gz
    for tz in range(2):
        for ty in range(2):
            acc = jnp.zeros((PAIR, 2 * PAIR), jnp.float32)
            for t, chunk in enumerate(chunks):
                columns = []
                for tx in range(2):
                    column = []
                    for e in chunk:
                        ex, ey, ez = OFFSETS[e]
                        for h in range(2):
                            code = (
                                49 * (2 * ex + h - tx + 3)
                                + 7 * (2 * ey - ty + 3)
                                + (2 * ez - tz + 3)
                            )
                            column.append(m0[base + code])
                    columns.append(jnp.concatenate(column, axis=0))
                weights = jnp.concatenate(columns, axis=1)
                acc = acc + jnp.dot(
                    xt[t, :, : len(chunk) * RANK], weights, preferred_element_type=jnp.float32
                )
            first = acc[:COLS, :PAIR] + pltpu.roll(acc[COLS:, :PAIR], COLS, 1)
            second = pltpu.roll(acc[:COLS, PAIR:], COLS, 1) + acc[COLS:, PAIR:]
            sum_send[2 * tz + ty, :COLS, :] = jnp.where(lanes < COLS, first, second)

    for_each(clusters, lambda i, dev: clus_copy(i, i, me).wait_recv())
    acc = jnp.zeros((PAIR, PAIR), jnp.float32)
    for t in range(2):
        column = []
        for i in range(8 * t, 8 * t + 8):
            column.append(m1[cluster_base + clusters[i][2]])
        rows = x1[pl.ds(8 * t, 8)].reshape(8 * HALF, PAIR)
        acc = acc + jnp.dot(
            rows.T, jnp.concatenate(column, axis=0), preferred_element_type=jnp.float32
        )
    down = acc[:COLS] + pltpu.roll(acc[COLS:], COLS, 1)
    down = jnp.where(lanes[:HALF] < COLS, down[:HALF], pltpu.roll(down[HALF:], COLS, 1))
    for n in range(4):
        sum_send[n, COLS:, :] = down

    def sum_copy(r):
        return pltpu.make_async_remote_copy(
            src_ref=sum_send.at[(g + r) % 4],
            dst_ref=sum_recv.at[r - 1],
            send_sem=sum_send_sem.at[r - 1],
            recv_sem=sum_recv_sem.at[r - 1],
            device_id=(mates[r - 1],),
            device_id_type=MESH,
        )

    for r in range(1, 4):
        sum_copy(r).start()

    for d in range(2):
        for a in range(3):
            for n in range(3):
                run_if(
                    both(side_y[1 - d][1], layer_ok[a], spans[n][2]), copy_y(d, a, n).wait_recv
                )
    load_near.wait()
    load_list.wait()

    def slot_of(entry):
        lx = ((entry >> 0) & 1) + 2 * ((entry >> 3) & 1) + 4 * ((entry >> 6) & 1)
        ly = ((entry >> 1) & 1) + 2 * ((entry >> 4) & 1) + 4 * ((entry >> 7) & 1)
        lz = ((entry >> 2) & 1) + 2 * ((entry >> 5) & 1) + 4 * ((entry >> 8) & 1)
        slot = ((ly - y + 1) * 3 + lz - z + 1) * 4 + lx - 2 * bx + 1
        return jnp.where(entry < 0, ZERO_SLOT, jnp.clip(slot, 0, ZERO_SLOT))

    near_terms = []
    for h in range(2):
        acc = jnp.zeros((COLS, LEAF), jnp.float32)
        for k in range(NNEAR):
            acc = acc + jnp.dot(
                pbuf[slot_of(list_ref[h, k])], nbuf[h, k], preferred_element_type=jnp.float32
            )
        near_terms.append(acc)

    for r in range(1, 4):
        sum_copy(r).wait_recv()
    sums = sum_send[g] + sum_recv[0] + sum_recv[1] + sum_recv[2]
    down = jnp.concatenate([sums[COLS:, :COLS], sums[COLS:, COLS:]], axis=0).astype(jnp.bfloat16)
    for h in range(2):
        far_coef = sums[:COLS, COLS * h : COLS * (h + 1)] + lax.dot_general(
            down,
            transfer_vmem[h],
            (((1,), (1,)), ((), ())),
            preferred_element_type=jnp.float32,
        )
        far_term = jnp.dot(
            far_coef.astype(jnp.bfloat16), basis_vmem[h], preferred_element_type=jnp.float32
        )
        out_ref[h] = (near_terms[h] + far_term).astype(jnp.bfloat16)

    for r in range(1, 4):
        part_copy(r).wait_send()
        sum_copy(r).wait_send()

    coef_jobs = [coef_to_z(d) for d in range(2)]
    coef_jobs += [coef_to_y(d, a) for d in range(2) for a in range(3)]
    coef_jobs += [coef_to_x(d, a, n) for d in range(2) for a in range(3) for n in range(3)]
    for flag, copy in coef_jobs:
        run_if(flag, copy.wait_send)
    for_each(clusters, lambda i, dev: clus_copy(i, parent // 4, dev).wait_send())
    for flag, copy in panel_jobs():
        run_if(flag, copy.wait_send)


def per_device(panels, basis, transfer, near_blocks, coupling, near_list):
    tables = coupling.reshape(2, SHIFTS, HALF, PAIR).transpose(1, 2, 0, 3)
    tables = tables.reshape(SHIFTS, RANK, PAIR)
    vmem = pl.BlockSpec(memory_space=pltpu.VMEM)
    hbm = pl.BlockSpec(memory_space=pltpu.HBM)
    dma = pltpu.SemaphoreType.DMA
    return pl.pallas_call(
        kernel,
        name="h2_product",
        out_shape=jax.ShapeDtypeStruct((2, COLS, LEAF), jnp.bfloat16),
        in_specs=[hbm] * 6,
        out_specs=vmem,
        scratch_shapes=[
            pltpu.VMEM((37, COLS, LEAF), jnp.bfloat16),
            pltpu.VMEM((2, NNEAR, LEAF, LEAF), jnp.bfloat16),
            pltpu.SMEM((2, NNEAR), jnp.int32),
            pltpu.VMEM((2, RANK, LEAF), jnp.bfloat16),
            pltpu.VMEM((2, RANK, RANK), jnp.bfloat16),
            pltpu.VMEM((SHIFTS, RANK, PAIR), jnp.bfloat16),
            pltpu.VMEM((SHIFTS, HALF, PAIR), jnp.bfloat16),
            pltpu.VMEM((SHIFTS, HALF, PAIR), jnp.bfloat16),
            pltpu.VMEM((27, RANK, PAIR), jnp.bfloat16),
            pltpu.VMEM((16, HALF, PAIR), jnp.bfloat16),
            pltpu.VMEM((HALF, PAIR), jnp.bfloat16),
            pltpu.VMEM((HALF, PAIR), jnp.float32),
            pltpu.VMEM((3, HALF, PAIR), jnp.float32),
            pltpu.VMEM((4, COLS + HALF, PAIR), jnp.float32),
            pltpu.VMEM((3, COLS + HALF, PAIR), jnp.float32),
            pltpu.VMEM((RANK, COLS), jnp.float32),
            pltpu.VMEM((GROUP * RANK, PAIR), jnp.float32),
            pltpu.VMEM((7, PAIR, 2 * PAIR), jnp.bfloat16),
            dma((6,)),
            dma((27,)),
            dma((27,)),
            dma((27,)),
            dma((27,)),
            dma((3,)),
            dma((3,)),
            dma((16,)),
            dma((16,)),
            dma((3,)),
            dma((3,)),
        ],
        compiler_params=pltpu.CompilerParams(
            collective_id=0, has_side_effects=True, vmem_limit_bytes=48 << 20
        ),
    )(*[pltpu.with_memory_space_constraint(a, pltpu.HBM) for a in (panels, basis, transfer, near_blocks, tables, near_list)])


def solution(mesh):
    return jax.shard_map(
        per_device,
        mesh=mesh,
        in_specs=(
            P(AXIS, None, None),
            P(AXIS, None, None),
            P(AXIS, None, None),
            P(AXIS, None, None, None),
            P(),
            P(AXIS, None),
        ),
        out_specs=P(AXIS, None, None),
        check_vma=False,
    )
```
